32 devices in a mesh: fsdp: 16 (over z, x, core), tp: 2 (over y).
Axes of the slice: x: 2, y: 2, z: 4, core: 2. Of those that a mesh axis runs over, the one named last changes fastest.
Arguments:
- tokens: bfloat16 [2048, 3584], P('fsdp', 'tp'), may hold values from -6 to 6
- norm_gain: bfloat16 [3584], replicated, may hold values from 0.5 to 1.5
- gate_weight: bfloat16 [3584, 10240], P('fsdp', 'tp'), may hold values from -0.09375 to 0.09375
- up_weight: bfloat16 [3584, 10240], P('fsdp', 'tp'), may hold values from -0.09375 to 0.09375
- down_weight: bfloat16 [3584, 10240], P('fsdp', 'tp'), may hold values from -0.0625 to 0.0625
- probes: bfloat16 [2, 3584, 10240], P(None, 'fsdp', 'tp'), may hold values from -0.0625 to 0.0625
Outputs:
- layer_out: bfloat16 [2048, 3584], P('tp', 'fsdp')
- token_curv: float32 [2048], P('tp')
The draws below stay inside these ranges and needn't reach their ends.
All inputs are finite; a program needn't handle non-finite values.
Results may differ from the reference program's by a relative error of at most 0.014.
Values may be sent and summed in bfloat16 or wider, within the bound.
A program may use at most 128 MiB of HBM per device.

```python
import jax
import jax.numpy as jnp
from jax import lax

D = 3584
FF = 10240
PROBES = 2
TOKENS = 2048
N_TP = 2


def level_of(rng, dims, cuts, smallest, largest):
    def one(dim, parts):
        steps = jax.random.uniform(jax.random.fold_in(jax.random.fold_in(rng, 6), dim), (parts,), jnp.float32, smallest / len(cuts), largest / len(cuts))
        return jnp.repeat(jnp.exp(steps), dims[dim] // parts).reshape((-1,) + (1,) * (len(dims) - dim - 1))

    gain = one(*cuts[0])
    for cut in cuts[1:]:
        gain = gain * one(*cut)
    return gain


def bell_draw(own_key, dims, width, most, shards=(), dtype=jnp.bfloat16):
    factor_of = level_of(own_key, dims, shards, -0.22, 0.18) if shards else 1.0
    entries = jax.random.normal(own_key, dims, jnp.float32) * width * factor_of
    return jnp.minimum(jnp.maximum(entries, -most), most).astype(dtype)


def setup_inputs(seed: int = 0) -> dict:
    arg_keys = jax.random.split(jax.random.key(seed), 7)
    return {
        "tokens": bell_draw(arg_keys[0], (TOKENS, D), 1.0, 6.0, ((0, 16), (1, 2))),
        "norm_gain": jnp.clip(1.0 + 0.1 * jax.random.normal(arg_keys[1], (D,), jnp.float32), 0.5, 1.5).astype(jnp.bfloat16),
        "gate_weight": bell_draw(arg_keys[2], (D, FF), D ** -0.5, 0.09375, ((0, 16), (1, 2))),
        "up_weight": bell_draw(arg_keys[3], (D, FF), D ** -0.5, 0.09375, ((0, 16), (1, 2))),
        "down_weight": bell_draw(arg_keys[4], (D, FF), FF ** -0.5, 0.0625, ((0, 16), (1, 2))),
        "probes": bell_draw(arg_keys[5], (PROBES, D, FF), FF ** -0.5, 0.0625, ((1, 16), (2, 2))),
    }


epsilon = 1e-06

def reference(tokens, norm_gain, gate_weight, up_weight, down_weight, probes):
    widened = tokens.astype(jnp.float32)
    inverse_rms = lax.rsqrt(lax.optimization_barrier(jnp.mean(widened * widened, axis=1, keepdims=True)) + epsilon)
    normed = (widened * inverse_rms * norm_gain.astype(jnp.float32)).astype(jnp.bfloat16)
    gate_sum = jnp.dot(normed, gate_weight, preferred_element_type=jnp.float32)
    up_sum = jnp.dot(normed, up_weight, preferred_element_type=jnp.float32)
    hidden = (jax.nn.silu(gate_sum) * up_sum).astype(jnp.bfloat16)
    stacked = jnp.concatenate([down_weight[None], probes], axis=0)
    count = stacked.shape[0]
    block_width = FF // N_TP

    def add_block(block_index, running):
        offset = (block_index * block_width).astype(jnp.int32)
        columns = lax.dynamic_slice_in_dim(hidden, offset, block_width, 1)
        matrices = lax.dynamic_slice_in_dim(stacked, offset, block_width, 2)
        terms = [lax.dot_general(columns, matrices[which], (((1,), (1,)), ((), ())), preferred_element_type=jnp.float32).astype(jnp.bfloat16).astype(jnp.float32) for which in range(count)]
        return running + jnp.stack(terms)
    projected = lax.fori_loop(0, N_TP, add_block, jnp.zeros((count, TOKENS, D), jnp.float32))
    primal = projected[0]
    squashed = jax.nn.sigmoid(primal)
    slope = squashed * (1.0 - squashed)
    tangent_sq = lax.optimization_barrier(jnp.sum(projected[1:] * projected[1:], axis=0))
    token_curv = lax.optimization_barrier(jnp.sum(slope * tangent_sq, axis=1)) / (PROBES * D)
    return (primal.astype(jnp.bfloat16), token_curv)
```

```python
import jax
import jax.numpy as jnp
from jax import lax
from jax.experimental import pallas as pl
from jax.experimental.pallas import tpu as pltpu
from jax.sharding import PartitionSpec as P

D = 3584
PROBES = 2
MESH = pl.DeviceIdType.MESH
ANY = pl.BlockSpec(memory_space=pl.ANY)


epsilon = 1e-06


def remote(src, dst, send, recv, device):
    return pltpu.make_async_remote_copy(
        src_ref=src,
        dst_ref=dst,
        send_sem=send,
        recv_sem=recv,
        device_id=device,
        device_id_type=MESH,
    )


def exchange_kernel(chips, t_ref, g_ref, u_ref, to, go, uo, bounce, t_bounce, w_send, w_recv, c_send, c_recv, t_send, t_recv, local_sem):
    me = lax.axis_index("fsdp")
    tp = lax.axis_index("tp")
    chip, core = me // 2, me % 2
    outer, inner = chip // 2, chip % 2
    outers = chips // 2
    rows, width = go.shape[2], go.shape[3]
    t_rows, t_cols = t_ref.shape
    partner = {"fsdp": chip * 2 + 1 - core}
    across = {"tp": 1 - tp}

    barrier = pltpu.get_barrier_semaphore()
    for d in range(1, chips):
        pl.semaphore_signal(barrier, inc=1, device_id={"fsdp": ((chip + d) % chips) * 2 + core}, device_id_type=MESH)
    pl.semaphore_signal(barrier, inc=1, device_id=partner, device_id_type=MESH)
    pl.semaphore_signal(barrier, inc=1, device_id=across, device_id_type=MESH)
    pl.semaphore_wait(barrier, chips + 1)

    def token_slot(half, owner):
        return to.at[pl.ds(pl.multiple_of(owner * t_rows, t_rows), t_rows), pl.ds(pl.multiple_of(half * t_cols, 128), t_cols)]

    def token_copy(src, half, owner, way, device):
        return remote(src, token_slot(half, owner), t_send.at[way, owner], t_recv.at[half, owner], device)

    down = {"fsdp": (chip - 2) * 2 + core}
    up = {"fsdp": (chip + 2) * 2 + core}
    side = {"fsdp": (outer * 2 + 1 - inner) * 2 + core}

    def pass_on(src, owner, first):
        if first in (0, 1):
            @pl.when(outer > 0)
            def _():
                token_copy(src, tp, owner, 0, down).start()
        if first in (0, 2):
            @pl.when(outer < outers - 1)
            def _():
                token_copy(src, tp, owner, 1, up).start()
        token_copy(src, tp, owner, 2, side).start()
        token_copy(src, tp, owner, 3, across).start()

    pass_on(t_ref, chip, 0)
    weights = ((g_ref, go), (u_ref, uo))
    order = sorted(range(1, chips), key=lambda d: -min(d // 2, (chips - d) // 2))
    sends = [(a, d) for a in range(2) for d in order]

    def weight_send(a, d):
        src, dst = weights[a]
        peer = (chip + d) % chips
        return remote(
            src.at[:, pl.ds(pl.multiple_of(peer * width, 128), width)],
            dst.at[chip, core],
            w_send.at[a, d],
            w_recv.at[a, chip],
            {"fsdp": peer * 2 + core},
        )

    batch = -(-len(sends) // outers)
    batches = [sends[i * batch : (i + 1) * batch] for i in range(outers)]
    for a, d in batches[0]:
        weight_send(a, d).start()

    def own(a):
        return weights[a][0].at[:, pl.ds(pl.multiple_of(chip * width, 128), width)]

    def own_out(a):
        return remote(own(a), weights[a][1].at[chip, core], c_send.at[a, chip], c_recv.at[a, chip], partner)

    for a in range(2):
        own_out(a).start()
        pltpu.make_async_copy(own(a), bounce.at[a], local_sem.at[a]).start()
    pltpu.make_async_copy(t_ref, t_bounce, local_sem.at[2]).start()
    for a in range(2):
        pltpu.make_async_copy(own(a), bounce.at[a], local_sem.at[a]).wait()
        pltpu.make_async_copy(bounce.at[a], weights[a][1].at[chip, core], local_sem.at[a]).start()
    pltpu.make_async_copy(t_ref, t_bounce, local_sem.at[2]).wait()
    pltpu.make_async_copy(t_bounce, token_slot(tp, chip), local_sem.at[2]).start()

    def token_wait(half, owner):
        slot = token_slot(half, owner)
        remote(slot, slot, t_send.at[3, owner], t_recv.at[half, owner], across).wait_recv()

    for r in range(1, outers):
        @pl.when(outer - r >= 0)
        def _():
            owner = chip - 2 * r
            token_wait(tp, owner)
            pass_on(token_slot(tp, owner), owner, 2)

        @pl.when(outer + r < outers)
        def _():
            owner = chip + 2 * r
            token_wait(tp, owner)
            pass_on(token_slot(tp, owner), owner, 1)

        for a, d in batches[r]:
            weight_send(a, d).start()

    def side_owner(z):
        return z * 2 + 1 - inner

    def weight_wait_forward(a, d):
        s = (chip + chips - d) % chips
        block = weights[a][1].at[s, core]
        remote(block, block, w_send.at[a, d], w_recv.at[a, s], partner).wait_recv()
        remote(block, block, c_send.at[a, s], c_recv.at[a, s], partner).start()

    for a, d in batches[0]:
        weight_wait_forward(a, d)
    for z in range(outers):
        owner = side_owner(z)
        token_wait(tp, owner)
        slot = token_slot(tp, owner)
        token_copy(slot, tp, owner, 3, across).start()
    for group in batches[1:]:
        for a, d in group:
            weight_wait_forward(a, d)
    for s in range(chips):
        token_wait(1 - tp, s)
        for a in range(2):
            block = weights[a][1].at[s, 1 - core]
            remote(block, block, c_send.at[a, s], c_recv.at[a, s], partner).wait_recv()

    def sent(owner, way):
        slot = token_slot(tp, owner)
        remote(slot, slot, t_send.at[way, owner], t_recv.at[tp, owner], across).wait_send()

    for a, d in sends:
        weight_send(a, d).wait_send()
    for s in range(chips):
        for a in range(2):
            block = weights[a][1].at[s, core]
            remote(block, block, c_send.at[a, s], c_recv.at[a, s], partner).wait_send()
        sent(s, 3)
    for r in range(outers):
        @pl.when(outer - r >= 0)
        def _():
            owner = chip - 2 * r
            sent(owner, 2)

            @pl.when(outer < outers - 1)
            def _():
                sent(owner, 1)

        @pl.when(outer + r < outers)
        def _():
            owner = chip + 2 * r
            if r > 0:
                sent(owner, 2)

            @pl.when(outer > 0)
            def _():
                sent(owner, 0)
    for a in range(2):
        pltpu.make_async_copy(bounce.at[a], weights[a][1].at[chip, core], local_sem.at[a]).wait()
    pltpu.make_async_copy(t_bounce, token_slot(tp, chip), local_sem.at[2]).wait()


def exchange(tokens, gate_weight, up_weight, chips):
    rows, columns = gate_weight.shape
    width = columns // chips
    t_rows, t_cols = tokens.shape
    weight = jax.ShapeDtypeStruct((chips, 2, rows, width), gate_weight.dtype)
    pieces = pltpu.SemaphoreType.DMA((2, chips))
    t, g, u = pl.pallas_call(
        lambda *refs: exchange_kernel(chips, *refs),
        out_shape=(jax.ShapeDtypeStruct((chips * t_rows, 2 * t_cols), tokens.dtype), weight, weight),
        in_specs=[ANY] * 3,
        out_specs=[ANY] * 3,
        scratch_shapes=[
            pltpu.VMEM((2, rows, width), gate_weight.dtype),
            pltpu.VMEM((t_rows, t_cols), tokens.dtype),
            pieces,
            pieces,
            pieces,
            pieces,
            pltpu.SemaphoreType.DMA((4, chips)),
            pieces,
            pltpu.SemaphoreType.DMA((3,)),
        ],
        compiler_params=pltpu.CompilerParams(collective_id=1, has_side_effects=True),
        name="exchange",
    )(tokens, gate_weight, up_weight)
    return t, g.reshape(-1, width), u.reshape(-1, width)


def norm(features, norm_gain):
    widened = features.astype(jnp.float32)
    inverse_rms = lax.rsqrt(jnp.mean(widened * widened, axis=1, keepdims=True) + epsilon)
    return (widened * inverse_rms * norm_gain.astype(jnp.float32)).astype(jnp.bfloat16)


def dot(a, b):
    return jnp.dot(a, b, preferred_element_type=jnp.float32)


def project(hidden_all, down_weight, probes):
    stacked = jnp.concatenate([down_weight[None], probes], axis=0)
    count = stacked.shape[0]
    col_width = stacked.shape[1]
    flat_weights = stacked.reshape(count * col_width, stacked.shape[2])
    partial_terms = lax.dot_general(
        hidden_all,
        flat_weights,
        (((1,), (1,)), ((), ())),
        preferred_element_type=jnp.float32,
    )
    summed = lax.psum_scatter(
        partial_terms.astype(jnp.bfloat16), "tp", scatter_dimension=0, tiled=True
    ).astype(jnp.float32)
    summed_parts = summed.reshape(summed.shape[0], count, col_width)
    primal = summed_parts[:, 0, :]
    tangents = summed_parts[:, 1:, :]
    squashed = jax.nn.sigmoid(primal)
    slope = squashed * (1.0 - squashed)
    tangent_sq = jnp.sum(tangents * tangents, axis=1)
    local_curv = jnp.sum(slope * tangent_sq, axis=1) / (PROBES * D)
    token_curv = lax.psum(local_curv, "fsdp")
    return (primal.astype(jnp.bfloat16), token_curv)


def gathered_weights(tokens, norm_gain, gate_weight, up_weight, down_weight, probes):
    normed = norm(lax.all_gather(tokens, "tp", axis=1, tiled=True), norm_gain)
    gate_sum = dot(normed, lax.all_gather(gate_weight, "fsdp", axis=0, tiled=True))
    up_sum = dot(normed, lax.all_gather(up_weight, "fsdp", axis=0, tiled=True))
    hidden = (jax.nn.silu(gate_sum) * up_sum).astype(jnp.bfloat16)
    return project(lax.all_gather(hidden, "fsdp", axis=0, tiled=True), down_weight, probes)


def moved_weights(tokens, norm_gain, gate_weight, up_weight, down_weight, probes):
    chips = lax.axis_size("fsdp") // 2
    features, gate, up = exchange(tokens, gate_weight, up_weight, chips)
    normed = norm(features, norm_gain)
    hidden = (jax.nn.silu(dot(normed, gate)) * dot(normed, up)).astype(jnp.bfloat16)
    blocks = lax.all_gather(hidden, "fsdp", axis=0)
    t_rows, width = tokens.shape[0], hidden.shape[1]
    blocks = blocks.reshape(chips, 2, chips, t_rows, width)
    hidden_all = blocks.transpose(2, 1, 3, 0, 4).reshape(2 * chips * t_rows, chips * width)
    return project(hidden_all, down_weight, probes)


def solution(mesh):
    def on_device(tokens, norm_gain, gate_weight, up_weight, down_weight, probes):
        chips = mesh.shape["fsdp"] // 2
        fits = mesh.shape["tp"] == 2 and chips % 2 == 0 and gate_weight.shape[1] % (128 * chips) == 0 and tokens.shape[1] % 128 == 0
        form = moved_weights if fits else gathered_weights
        return form(tokens, norm_gain, gate_weight, up_weight, down_weight, probes)

    return jax.shard_map(
        on_device,
        mesh=mesh,
        in_specs=(
            P("fsdp", "tp"),
            P(),
            P("fsdp", "tp"),
            P("fsdp", "tp"),
            P("fsdp", "tp"),
            P(None, "fsdp", "tp"),
        ),
        out_specs=(P("tp", "fsdp"), P("tp")),
        check_vma=False,
    )
```
